32 devices in a mesh: dp: 16 (over z, y, core), tensor: 2 (over x).
Axes of the slice: x: 2, y: 2, z: 4, core: 2. Of those that a mesh axis runs over, the one named last changes fastest.
Arguments:
- tokens: bfloat16 [12288, 2048], P('dp'), may hold values from -6 to 6
- cotangent: bfloat16 [12288, 2048], P('dp'), may hold values from -8 to 8
- w_query: float32 [2048, 2048], P('dp', 'tensor'), may hold values from -0.125 to 0.125
- w_keyval: float32 [2048, 256], P('dp'), may hold values from -0.125 to 0.125
- w_out: float32 [2048, 2048], P('dp', 'tensor'), may hold values from -1 to 1
- w_up: float32 [2048, 8192], P('dp', 'tensor'), may hold values from -0.125 to 0.125
- w_down: float32 [2048, 8192], P('dp', 'tensor'), may hold values from -0.0625 to 0.0625
- norm1_gain: float32 [2048], P('dp'), may hold values from 0.25 to 1.75
- norm1_bias: float32 [2048], P('dp'), may hold values from -3 to 3
- norm2_gain: float32 [2048], P('dp'), may hold values from 0.25 to 1.75
- norm2_bias: float32 [2048], P('dp'), may hold values from -3 to 3
- route: int32 [12288], replicated, may hold values from 0 to 12287, as said below
- lengths: int32 [16, 4], P('dp'), may hold values from 1 to 512, 768 in all within a row
Outputs:
- output: bfloat16 [12288, 2048], P('dp')
- grad_tokens: bfloat16 [12288, 2048], P('dp')
- grad_w_query: float32 [2048, 2048], P('dp', 'tensor')
- grad_w_keyval: float32 [2048, 256], P('dp')
- grad_w_out: float32 [2048, 2048], P('dp', 'tensor')
- grad_w_up: float32 [2048, 8192], P('dp', 'tensor')
- grad_w_down: float32 [2048, 8192], P('dp', 'tensor')
- grad_norm1_gain: float32 [2048], P('dp')
- grad_norm1_bias: float32 [2048], P('dp')
- grad_norm2_gain: float32 [2048], P('dp')
- grad_norm2_bias: float32 [2048], P('dp')
The draws below stay inside these ranges and needn't reach their ends.
Inputs may be any that keep to these rules, and one draw needn't show every extreme that they name: route is a permutation of the 12288 places; places g * 768 to (g + 1) * 768 - 1 belong to index g of dp, and the 768 tokens of each index of dp name exactly 48 places of every index of dp. Row g lists the lengths of the 4 sequences at index g of dp in order; they sum to 768, and the longest of each row is exactly 512.
All inputs are finite; a program needn't handle non-finite values.
Results may differ from the reference program's by a relative error of at most 0.012.
The reference program's roundings to bfloat16 on the way count: a program that leaves them out, or rounds other values in their place, can miss the bound.
Values may be sent and summed in bfloat16 or wider, within the bound.
A program may use at most 320 MiB of HBM per device.

```python
import math
from functools import partial
import jax
import jax.numpy as jnp
import numpy as np
from jax import lax

D = 2048
HEADS = 16
HD = 128
FF = 8192
TOK_DEV = 768
SEQ_DEV = 4
MAXLEN = 512
TOKENS = 12288
N_DP = 16


def draw_route(key, part):
    groups = TOKENS // TOK_DEV
    pair_rows = TOK_DEV // groups

    def shuffle_slots(slot_key):
        return jax.random.permutation(slot_key, TOK_DEV).astype(jnp.int32)
    slot_keys = jax.random.split(jax.random.fold_in(key, 11), groups)
    shuffled = jax.vmap(shuffle_slots)(slot_keys)
    source_of_slot = (shuffled // pair_rows).reshape(TOKENS).astype(jnp.int32)
    slot_ids = jnp.arange(TOKENS, dtype=jnp.int32)
    by_source = slot_ids[jnp.argsort(source_of_slot, stable=True).astype(jnp.int32)]
    token_keys = jax.random.split(jax.random.fold_in(key, 12), groups)
    placing = jax.vmap(shuffle_slots)(token_keys)
    targets = (jnp.arange(groups, dtype=jnp.int32)[:, None] * TOK_DEV + placing).reshape(TOKENS).astype(jnp.int32)
    return jnp.zeros((TOKENS,), jnp.int32).at[targets].set(by_source)


def strengthened(values, stream_key, source, target, blocks, factor):
    def block_of(dim):
        return (jnp.arange(values.shape[dim]) // (values.shape[dim] // blocks)).reshape((-1,) + (1,) * (values.ndim - 1 - dim))

    near = jax.random.permutation(stream_key, blocks)[block_of(target)]
    second = (block_of(target) + blocks // 2) % blocks
    return jnp.where((block_of(source) == near) | (block_of(source) == second), factor * values, values)


def block_scale(key, shape, pieces, least, top_value):
    loudness, own = 1.0, jax.random.fold_in(key, 6)
    for axis_at, parts in pieces:
        steps = jnp.exp(jax.random.uniform(jax.random.fold_in(own, axis_at), (parts,), jnp.float32, least / len(pieces), top_value / len(pieces)))
        loudness = loudness * jnp.repeat(steps, shape[axis_at] // parts).reshape([-1 if axis == axis_at else 1 for axis in range(len(shape))])
    return loudness


def split_up(count, total, limit, skew):
    weights = [(1 << 20) // math.isqrt(standing ** skew) + 1 for standing in range(2, count + 1)]
    surplus, counts = total - limit - (count - 1), [1] * (count - 1)
    while surplus > 0:
        movable = [i for i in range(count - 1) if counts[i] < limit]
        whole, budget = sum([weights[i] for i in movable]), surplus
        for i in movable:
            more = min(limit - counts[i], max(1, budget * weights[i] // whole), surplus)
            counts[i] = counts[i] + more
            surplus = surplus - more
    return np.array([limit] + counts)


def uneven(rng, amount, total, most, skew):
    if amount == 2:
        one = jax.random.randint(rng, (), max(1, total - most), min(most, total - 1) + 1)
        return jnp.stack([one, total - one])
    sizes = jnp.asarray(split_up(amount, total, most, skew), jnp.int32)
    twos = (amount - 1) // 2
    source_of, sink = sizes[1:1 + 2 * twos:2], sizes[2:2 + 2 * twos:2]
    slack = jnp.minimum(source_of - 1, most - sink)
    moved = jax.random.randint(jax.random.fold_in(rng, 1), (twos,), 0, 1 << 20) % (slack + 1)
    sizes = sizes.at[1:1 + 2 * twos:2].set(source_of - moved).at[2:2 + 2 * twos:2].set(sink + moved)
    return sizes[jax.random.permutation(jax.random.fold_in(rng, 2), amount)]


def noise(key, dims, deviation, reach, shards=(), kind=jnp.bfloat16):
    values = jax.random.normal(key, dims, jnp.float32) * deviation
    if len(shards) > 0:
        values = block_scale(key, dims, shards, -0.22, 0.18) * values
    return jnp.clip(values, min=-reach, max=reach).astype(kind)


def heavy_noise(rng, shape, scale, bound, pieces, heavy, held_as=jnp.bfloat16):
    entries = scale * jax.random.normal(rng, shape, jnp.float32)
    if pieces:
        entries = entries * block_scale(rng, shape, pieces, -0.22, 0.18)
    return jnp.clip(strengthened(entries, jax.random.fold_in(rng, 3), *heavy), -bound, bound).astype(held_as)


def setup_inputs(seed: int = 0) -> dict:
    splits = jax.random.split(jax.random.key(seed), 14)
    return {
        "tokens": noise(splits[0], (TOKENS, D), 1.0, 6.0, ((0, 16),)),
        "cotangent": heavy_noise(splits[1], (TOKENS, D), 1.0, 8.0, ((0, 16),), (0, 1, 16, 2.0)),
        "w_query": noise(splits[2], (D, D), D ** -0.5, 0.125, ((0, 16), (1, 2)), jnp.float32),
        "w_keyval": noise(splits[3], (D, 2 * HD), D ** -0.5, 0.125, ((0, 16),), jnp.float32),
        "w_out": noise(splits[4], (D, D), (max(D // 64, 8)) ** -0.5, 1.0, ((0, 16), (1, 2)), jnp.float32),
        "w_up": noise(splits[5], (D, FF), D ** -0.5, 0.125, ((0, 16), (1, 2)), jnp.float32),
        "w_down": noise(splits[6], (D, FF), FF ** -0.5, 0.0625, ((0, 16), (1, 2)), jnp.float32),
        "norm1_gain": jnp.clip(1.0 + 0.15 * jax.random.normal(splits[7], (D,), jnp.float32), 0.25, 1.75),
        "norm1_bias": noise(splits[8], (D,), 0.3, 3.0, ((0, 16),), jnp.float32),
        "norm2_gain": jnp.clip(1.0 + 0.15 * jax.random.normal(splits[9], (D,), jnp.float32), 0.25, 1.75),
        "norm2_bias": noise(splits[10], (D,), 0.3, 3.0, ((0, 16),), jnp.float32),
        "route": draw_route(jax.random.fold_in(splits[13], 71), 0),
        "lengths": jax.vmap(lambda own: uneven(own, SEQ_DEV, TOK_DEV, MAXLEN, 2))(jax.random.split(splits[12], N_DP)).reshape((N_DP, SEQ_DEV)).astype(jnp.int32),
    }


norm_eps = 1e-05
highest = lax.Precision.HIGHEST

@jax.custom_vjp
def low(v):
    return lax.optimization_barrier(v.astype(jnp.bfloat16)).astype(jnp.float32)

@jax.custom_vjp
def low_back(v):
    return v

def low_keep(v):
    return (low(v), None)

def low_pass(kept, grad):
    return (grad,)

def back_keep(v):
    return (v, None)

def back_low(kept, grad):
    return (low(grad),)
low.defvjp(low_keep, low_pass)
low_back.defvjp(back_keep, back_low)

def layer_norm(values, gain_vector, shift_vector):
    row_mean = lax.optimization_barrier(jnp.mean(values, axis=-1, keepdims=True))
    centered = values - row_mean
    spread = lax.optimization_barrier(jnp.mean(centered * centered, axis=-1, keepdims=True))
    return centered * lax.rsqrt(spread + norm_eps) * gain_vector + shift_vector

def matmul(first_op, second_op):
    return jnp.dot(first_op, second_op, precision=highest)

def visible_pairs(lengths_row, row_count):
    boundaries = jnp.cumsum(lengths_row).astype(jnp.int32)
    places = jnp.arange(row_count, dtype=jnp.int32)
    segment = lax.optimization_barrier(jnp.sum((places[:, None] >= boundaries[None, :]).astype(jnp.int32), axis=1)).astype(jnp.int32)
    return jnp.logical_and(segment[:, None] == segment[None, :], places[None, :] <= places[:, None])

def block_layer(lengths_row, resid_in, w_query, w_keyval, w_out, w_up, w_down, first_gain, first_shift, second_gain, second_shift):
    row_count = resid_in.shape[0]
    normed_one = low(layer_norm(resid_in, low(first_gain), low(first_shift)))
    queries = low(low_back(matmul(normed_one, low(w_query))))
    keyval = low(low_back(matmul(normed_one, low(w_keyval))))
    query_heads = queries.reshape(row_count, HEADS, HD)
    key_rows = keyval[:, :HD]
    value_rows = keyval[:, HD:]
    scores = low_back(jnp.einsum('qhd,kd->hqk', query_heads, key_rows, precision=highest) * HD ** (-0.5))
    visible = visible_pairs(lengths_row, row_count)
    masked = jnp.where(visible[None], scores, -1e+30)
    row_max = lax.optimization_barrier(jnp.max(masked, axis=2, keepdims=True))
    weights_exp = jnp.exp(masked - row_max)
    probabilities = weights_exp / lax.optimization_barrier(jnp.sum(weights_exp, axis=2, keepdims=True))
    context = jnp.einsum('hqk,kd->qhd', low(probabilities), value_rows, precision=highest)
    context = low(low_back(context.reshape(row_count, HEADS * HD)))
    resid_mid = resid_in + low_back(matmul(context, low(w_out).T))
    normed_two = low(layer_norm(resid_mid, low(second_gain), low(second_shift)))
    hidden_pre = low_back(matmul(normed_two, low(w_up)))
    active = low(jax.nn.gelu(hidden_pre, approximate=True))
    return resid_mid + matmul(active, low(w_down).T)

def reference(tokens, cotangent, w_query, w_keyval, w_out, w_up, w_down, norm1_gain, norm1_bias, norm2_gain, norm2_bias, route, lengths):
    inverse = jnp.argsort(route).astype(jnp.int32)
    routed_in = tokens.astype(jnp.float32)[inverse].reshape(N_DP, TOK_DEV, D)
    routed_grad = cotangent.astype(jnp.float32)[inverse].reshape(N_DP, TOK_DEV, D)
    masters = (w_query, w_keyval, w_out, w_up, w_down, norm1_gain, norm1_bias, norm2_gain, norm2_bias)

    def step(totals, operands):
        block_in, block_grad, lengths_row = operands
        result, backward = jax.vjp(partial(block_layer, lengths_row), block_in, *masters)
        gradients = backward(block_grad)
        return (jax.tree.map(jnp.add, totals, tuple(gradients[1:])), (result, gradients[0]))
    initial = jax.tree.map(jnp.zeros_like, masters)
    totals, outputs = lax.scan(step, initial, (routed_in, routed_grad, lengths))
    output = outputs[0].reshape(TOKENS, D)[route].astype(jnp.bfloat16)
    grad_tokens = outputs[1].reshape(TOKENS, D)[route].astype(jnp.bfloat16)
    return (output, grad_tokens, totals[0], totals[1], totals[2], totals[3], totals[4], totals[5], totals[6], totals[7], totals[8])
```

```python
import jax
import jax.numpy as jnp
from jax import lax
from jax.sharding import PartitionSpec as P

norm_eps = 1e-05


def layer_norm(values, gain_vector, shift_vector):
    row_mean = jnp.mean(values, axis=-1, keepdims=True)
    centered = values - row_mean
    spread = jnp.mean(centered * centered, axis=-1, keepdims=True)
    return centered * lax.rsqrt(spread + norm_eps) * gain_vector + shift_vector


def gelu_tanh(values):
    return jax.nn.gelu(values, approximate=True)


def visible_pairs(lengths_row, row_count):
    boundaries = jnp.cumsum(lengths_row)
    places = jnp.arange(row_count, dtype=jnp.int32)
    segment = jnp.sum((places[:, None] >= boundaries[None, :]).astype(jnp.int32), axis=1)
    return jnp.logical_and(segment[:, None] == segment[None, :], places[None, :] <= places[:, None])


def right_product(first_op, second_op):
    return lax.dot_general(
        first_op, second_op, (((1,), (1,)), ((), ())), preferred_element_type=jnp.float32
    )


def left_product(first_op, second_op):
    return lax.dot_general(
        first_op, second_op, (((0,), (0,)), ((), ())), preferred_element_type=jnp.float32
    )


def as_columns(vectors):
    columns = jnp.stack([vector.astype(jnp.bfloat16) for vector in vectors], axis=1)
    return jnp.pad(columns, ((0, 0), (0, 128 - len(vectors))))


def tensor_sum(values, ride_along=None):
    own = lax.optimization_barrier(values.astype(jnp.bfloat16))
    total = own.astype(jnp.float32)
    if lax.axis_size("tensor") == 2:
        other = lax.ppermute(own, "tensor", [(0, 1), (1, 0)])
        if ride_along is not None:
            other, ride_along = lax.optimization_barrier((other, ride_along))
        summed = total + other.astype(jnp.float32)
    else:
        summed = lax.psum(own, "tensor").astype(jnp.float32)
    return summed if ride_along is None else (summed, ride_along)


def summed_rows(low):
    total = lax.psum_scatter(low, "dp", scatter_dimension=0, tiled=True)
    return total.astype(jnp.float32)


def weight_term(first_op, second_op):
    return left_product(first_op, second_op).astype(jnp.bfloat16)


def masked_scores(query_heads, key_rows, visible, score_scale):
    scores = (
        jnp.einsum("qhd,kd->hqk", query_heads, key_rows, preferred_element_type=jnp.float32)
        * score_scale
    )
    return jnp.where(visible, scores, -1e30)


def per_device(
    tokens,
    cotangent,
    w_query,
    w_keyval,
    w_out,
    w_up,
    w_down,
    norm1_gain,
    norm1_bias,
    norm2_gain,
    norm2_bias,
    route,
    lengths,
):
    row_count = tokens.shape[0]
    head_dim = w_keyval.shape[1] // 2
    heads_here = w_query.shape[1] // head_dim
    score_scale = head_dim ** (-0.5)
    group_index = lax.axis_index("dp")
    first_block = jnp.concatenate(
        [
            w_query.astype(jnp.bfloat16),
            w_keyval.astype(jnp.bfloat16),
            as_columns((norm1_gain, norm1_bias, norm2_gain, norm2_bias)),
        ],
        axis=1,
    )
    full_first = lax.all_gather(first_block, "dp", axis=0, tiled=True)
    full_out = lax.all_gather(w_out.astype(jnp.bfloat16), "dp", axis=0, tiled=True)
    full_up = lax.all_gather(w_up.astype(jnp.bfloat16), "dp", axis=0, tiled=True)
    full_down = lax.all_gather(w_down.astype(jnp.bfloat16), "dp", axis=0, tiled=True)
    own_route = lax.dynamic_slice_in_dim(route, group_index * row_count, row_count)
    send_order = jnp.argsort(own_route, stable=True)
    inverse = jnp.argsort(route, stable=True)
    sources = lax.dynamic_slice_in_dim(inverse, group_index * row_count, row_count) // row_count
    recv_order = jnp.argsort(sources, stable=True)
    placing = jnp.argsort(recv_order, stable=True)
    arrived = (
        lax.all_to_all(tokens[send_order], "dp", split_axis=0, concat_axis=0, tiled=True),
        lax.all_to_all(cotangent[send_order], "dp", split_axis=0, concat_axis=0, tiled=True),
    )
    tokens_here = arrived[0][placing]
    grad_here = arrived[1][placing]
    qkv_cols = w_query.shape[1] + w_keyval.shape[1]
    full_qkv = full_first[:, :qkv_cols]
    norm_rows = full_first[:, qkv_cols : qkv_cols + 4].astype(jnp.float32).T
    first_gain, first_shift, second_gain, second_shift = (
        norm_rows[0],
        norm_rows[1],
        norm_rows[2],
        norm_rows[3],
    )
    resid_in = tokens_here.astype(jnp.float32)
    normed_one = layer_norm(resid_in, first_gain, first_shift).astype(jnp.bfloat16)
    qkv = jnp.dot(normed_one, full_qkv, preferred_element_type=jnp.float32).astype(jnp.bfloat16)
    query_heads = qkv[:, : w_query.shape[1]].reshape(row_count, heads_here, head_dim)
    key_rows = qkv[:, w_query.shape[1] : w_query.shape[1] + head_dim]
    value_rows = qkv[:, w_query.shape[1] + head_dim :]
    visible = visible_pairs(lengths[0], row_count)[None]
    masked = masked_scores(query_heads, key_rows, visible, score_scale)
    row_max = jnp.max(masked, axis=2, keepdims=True)
    weights_exp = jnp.exp(masked - row_max)
    row_total = jnp.sum(weights_exp, axis=2, keepdims=True)
    probs_first = (weights_exp / row_total).astype(jnp.bfloat16)
    log_total = row_max + jnp.log(row_total)
    context = jnp.einsum("hqk,kd->qhd", probs_first, value_rows, preferred_element_type=jnp.float32)
    context = context.reshape(row_count, heads_here * head_dim).astype(jnp.bfloat16)
    attn_output = tensor_sum(right_product(context, full_out))
    resid_mid = resid_in + attn_output
    normed_two = layer_norm(resid_mid, second_gain, second_shift).astype(jnp.bfloat16)
    hidden_pre = jnp.dot(normed_two, full_up, preferred_element_type=jnp.float32)
    active = gelu_tanh(hidden_pre).astype(jnp.bfloat16)
    grad_out = grad_here.astype(jnp.float32)
    grad_here, wdown_term = lax.optimization_barrier((grad_here, weight_term(grad_here, active)))
    grad_wdown = summed_rows(wdown_term)
    grad_active = jnp.dot(grad_here, full_down, preferred_element_type=jnp.float32)
    gelu_back = jax.vjp(gelu_tanh, hidden_pre)[1]
    grad_up = gelu_back(grad_active)[0].astype(jnp.bfloat16)
    norm_two_part = right_product(grad_up, full_up)
    grad_norm_two, wup_term = tensor_sum(norm_two_part, weight_term(normed_two, grad_up))
    grad_wup = summed_rows(wup_term)
    norm_two_back = jax.vjp(layer_norm, resid_mid, second_gain, second_shift)[1]
    grad_mid_norm, grad_gain_two, grad_shift_two = norm_two_back(grad_norm_two)
    grad_mid = grad_out + grad_mid_norm
    grad_mid_low = grad_mid.astype(jnp.bfloat16)
    grad_context = jnp.dot(grad_mid_low, full_out, preferred_element_type=jnp.float32)
    grad_context = grad_context.astype(jnp.bfloat16)
    grad_ctx_heads = grad_context.reshape(row_count, heads_here, head_dim)
    masked_again = masked_scores(query_heads, key_rows, visible, score_scale)
    probs_again = jnp.exp(masked_again - log_total)
    probs_low = probs_again.astype(jnp.bfloat16)
    grad_probs = jnp.einsum(
        "qhd,kd->hqk", grad_ctx_heads, value_rows, preferred_element_type=jnp.float32
    )
    row_delta = jnp.sum(grad_probs * probs_again, axis=2, keepdims=True)
    grad_scores = (probs_again * (grad_probs - row_delta)).astype(jnp.bfloat16)
    grad_query = (
        jnp.einsum("hqk,kd->qhd", grad_scores, key_rows, preferred_element_type=jnp.float32)
        * score_scale
    )
    grad_query = grad_query.reshape(row_count, heads_here * head_dim).astype(jnp.bfloat16)
    grad_keys = (
        jnp.einsum("hqk,qhd->kd", grad_scores, query_heads, preferred_element_type=jnp.float32)
        * score_scale
    )
    grad_values = jnp.einsum(
        "hqk,qhd->kd", probs_low, grad_ctx_heads, preferred_element_type=jnp.float32
    )
    grad_keyval_part = jnp.concatenate([grad_keys, grad_values], axis=1)
    grad_keyval_low = tensor_sum(grad_keyval_part).astype(jnp.bfloat16)
    grad_qkv_part = jnp.concatenate([grad_query, grad_keyval_part.astype(jnp.bfloat16)], axis=1)
    grad_norm_one, wo_term = tensor_sum(
        right_product(grad_qkv_part, full_qkv), weight_term(grad_mid_low, context)
    )
    grad_wo = summed_rows(wo_term)
    norm_one_back = jax.vjp(layer_norm, resid_in, first_gain, first_shift)[1]
    grad_in_norm, grad_gain_one, grad_shift_one = norm_one_back(grad_norm_one)
    grad_resid = (grad_mid + grad_in_norm).astype(jnp.bfloat16)
    mlp_output = tensor_sum(right_product(active, full_down))
    result = (resid_mid + mlp_output).astype(jnp.bfloat16)
    grad_qkv = jnp.concatenate([grad_query, grad_keyval_low], axis=1)
    last_rows = summed_rows(
        jnp.concatenate(
            [
                weight_term(normed_one, grad_qkv),
                as_columns((grad_gain_one, grad_shift_one, grad_gain_two, grad_shift_two)),
            ],
            axis=1,
        ),
    )
    norm_grads = last_rows[:, qkv_cols : qkv_cols + 4].T
    returned = (
        lax.all_to_all(result[recv_order], "dp", split_axis=0, concat_axis=0, tiled=True),
        lax.all_to_all(grad_resid[recv_order], "dp", split_axis=0, concat_axis=0, tiled=True),
    )
    restore = jnp.argsort(send_order, stable=True)
    output = returned[0][restore]
    grad_tokens = returned[1][restore]
    return (
        output,
        grad_tokens,
        last_rows[:, : w_query.shape[1]],
        last_rows[:, w_query.shape[1] : qkv_cols],
        grad_wo,
        grad_wup,
        grad_wdown,
        norm_grads[0],
        norm_grads[1],
        norm_grads[2],
        norm_grads[3],
    )


def solution(mesh):
    placed = (
        P("dp", None),
        P("dp", None),
        P("dp", "tensor"),
        P("dp", None),
        P("dp", "tensor"),
        P("dp", "tensor"),
        P("dp", "tensor"),
        P("dp"),
        P("dp"),
        P("dp"),
        P("dp"),
        P(),
        P("dp", None),
    )

    return jax.shard_map(
        per_device,
        mesh=mesh,
        in_specs=placed,
        out_specs=(
            P("dp", None),
            P("dp", None),
            P("dp", "tensor"),
            P("dp", None),
            P("dp", "tensor"),
            P("dp", "tensor"),
            P("dp", "tensor"),
            P("dp"),
            P("dp"),
            P("dp"),
            P("dp"),
        ),
        check_vma=False,
    )
```

```python
import jax
import jax.numpy as jnp
from jax import lax
from jax.sharding import PartitionSpec as P

norm_eps = 1e-05


def layer_norm(values, gain_vector, shift_vector):
    row_mean = jnp.mean(values, axis=-1, keepdims=True)
    centered = values - row_mean
    spread = jnp.mean(centered * centered, axis=-1, keepdims=True)
    return centered * lax.rsqrt(spread + norm_eps) * gain_vector + shift_vector


def gelu_tanh(values):
    return jax.nn.gelu(values, approximate=True)


def visible_pairs(lengths_row, places):
    boundaries = jnp.cumsum(lengths_row)
    segment = jnp.sum((places[:, None] >= boundaries[None, :]).astype(jnp.int32), axis=1)
    return jnp.logical_and(segment[:, None] == segment[None, :], places[None, :] <= places[:, None])


def right_product(first_op, second_op):
    return lax.dot_general(
        first_op, second_op, (((1,), (1,)), ((), ())), preferred_element_type=jnp.float32
    )


def left_product(first_op, second_op):
    return lax.dot_general(
        first_op, second_op, (((0,), (0,)), ((), ())), preferred_element_type=jnp.float32
    )


def as_columns(vectors):
    columns = jnp.stack([vector.astype(jnp.bfloat16) for vector in vectors], axis=1)
    return jnp.pad(columns, ((0, 0), (0, 128 - len(vectors))))


def tensor_sum(values, ride_along=None):
    own = lax.optimization_barrier(values.astype(jnp.bfloat16))
    total = own.astype(jnp.float32)
    other = swap_tensor(own)
    if ride_along is not None:
        other, ride_along = lax.optimization_barrier((other, ride_along))
    summed = total + other.astype(jnp.float32)
    return summed if ride_along is None else (summed, ride_along)


def swap_cores(values):
    members = lax.axis_size("dp")
    return lax.ppermute(values, "dp", [(i, i ^ 1) for i in range(members)])


def column_half(values, half):
    width = values.shape[1] // 2
    return lax.dynamic_slice_in_dim(values, half * width, width, axis=1)


def own_rows(values, part, parts):
    count = values.shape[0] // parts
    return lax.dynamic_slice_in_dim(values, part * count, count, axis=0)


def both_cores(values):
    return jnp.concatenate([values, swap_cores(values)], axis=0)


def half_of_both(values, core):
    other = swap_cores(column_half(values, 1 - core))
    return jnp.concatenate([column_half(values, core), other], axis=0)


def summed_rows(low):
    members = lax.axis_size("dp")
    groups = [list(range(core, members, 2)) for core in range(2)]
    return lax.psum_scatter(low, "dp", scatter_dimension=0, axis_index_groups=groups, tiled=True)


def own_columns(chip_rows, core):
    kept = own_rows(chip_rows, core, 2)
    other = swap_cores(own_rows(chip_rows, 1 - core, 2))
    first = jnp.where(core == 0, kept, other)
    second = jnp.where(core == 0, other, kept)
    return jnp.concatenate([first, second], axis=1).astype(jnp.float32)


def swap_tensor(values):
    return lax.ppermute(values, "tensor", [(0, 1), (1, 0)])


def tensor_rows(values, place):
    low = values.astype(jnp.bfloat16)
    arriving = swap_tensor(own_rows(low, 1 - place, 2))
    return own_rows(low, place, 2).astype(jnp.float32) + arriving.astype(jnp.float32)


def weight_term(first_op, second_op):
    return left_product(first_op, second_op).astype(jnp.bfloat16)


def masked_scores(query_heads, key_rows, visible, score_scale):
    scores = (
        jnp.einsum("qhd,kd->hqk", query_heads, key_rows, preferred_element_type=jnp.float32)
        * score_scale
    )
    return jnp.where(visible, scores, -1e30)


def per_device(
    tokens,
    cotangent,
    w_query,
    w_keyval,
    w_out,
    w_up,
    w_down,
    norm1_gain,
    norm1_bias,
    norm2_gain,
    norm2_bias,
    route,
    lengths,
):
    row_count = tokens.shape[0]
    head_dim = w_keyval.shape[1] // 2
    heads_here = w_query.shape[1] // head_dim
    score_scale = head_dim ** (-0.5)
    group_index = lax.axis_index("dp")
    groups = lax.axis_size("dp")
    core = lax.rem(group_index, 2)
    place = lax.axis_index("tensor")
    query_cols = w_query.shape[1]
    qkv_cols = query_cols + w_keyval.shape[1]
    up_cols = w_up.shape[1]
    full_attn = lax.all_gather(
        jnp.concatenate(
            [
                w_query.astype(jnp.bfloat16),
                w_keyval.astype(jnp.bfloat16),
                w_out.astype(jnp.bfloat16),
                as_columns((norm1_gain, norm1_bias, norm2_gain, norm2_bias)),
            ],
            axis=1,
        ),
        "dp",
        axis=0,
        tiled=True,
    )
    full_ffn = lax.all_gather(
        jnp.concatenate([w_up.astype(jnp.bfloat16), w_down.astype(jnp.bfloat16)], axis=1),
        "dp",
        axis=0,
        tiled=True,
    )
    full_up = full_ffn[:, :up_cols]
    full_down = full_ffn[:, up_cols:]

    def by_member(order):
        return order.reshape(groups, 2, -1).transpose(1, 0, 2)

    own_route = lax.dynamic_slice_in_dim(route, group_index * row_count, row_count)
    send_order = by_member(jnp.argsort(own_route, stable=True))
    own_sends = lax.dynamic_index_in_dim(send_order, place, keepdims=False).reshape(-1)

    def fetched(rows):
        mine = lax.all_to_all(rows[own_sends], "dp", split_axis=0, concat_axis=0, tiled=True)
        other = swap_tensor(mine)
        first = jnp.where(place == 0, mine, other)
        second = jnp.where(place == 0, other, mine)
        return jnp.concatenate([first, second], axis=0)

    tokens_here = fetched(tokens)
    grad_here = fetched(cotangent)
    inverse = jnp.argsort(route, stable=True)
    sources = lax.dynamic_slice_in_dim(inverse, group_index * row_count, row_count) // row_count
    places = by_member(jnp.argsort(sources, stable=True)).reshape(-1).astype(jnp.int32)
    full_qkv = full_attn[:, :qkv_cols]
    norm_at = qkv_cols + query_cols
    full_out = full_attn[:, qkv_cols:norm_at]
    norm_rows = full_attn[:, norm_at : norm_at + 4].astype(jnp.float32).T
    first_gain, first_shift, second_gain, second_shift = (
        norm_rows[0],
        norm_rows[1],
        norm_rows[2],
        norm_rows[3],
    )
    resid_in = tokens_here.astype(jnp.float32)
    normed_one = layer_norm(resid_in, first_gain, first_shift).astype(jnp.bfloat16)
    qkv = jnp.dot(normed_one, full_qkv, preferred_element_type=jnp.float32).astype(jnp.bfloat16)
    query_heads = qkv[:, :query_cols].reshape(row_count, heads_here, head_dim)
    key_rows = qkv[:, query_cols : query_cols + head_dim]
    value_rows = qkv[:, query_cols + head_dim :]
    visible = visible_pairs(lengths[0], places)[None]
    masked = masked_scores(query_heads, key_rows, visible, score_scale)
    row_max = jnp.max(masked, axis=2, keepdims=True)
    weights_exp = jnp.exp(masked - row_max)
    row_total = jnp.sum(weights_exp, axis=2, keepdims=True)
    probs_first = (weights_exp / row_total).astype(jnp.bfloat16)
    log_total = row_max + jnp.log(row_total)
    context = jnp.einsum("hqk,kd->qhd", probs_first, value_rows, preferred_element_type=jnp.float32)
    context = context.reshape(row_count, heads_here * head_dim).astype(jnp.bfloat16)
    attn_output = tensor_sum(right_product(context, full_out))
    resid_mid = resid_in + attn_output
    normed_two = layer_norm(resid_mid, second_gain, second_shift).astype(jnp.bfloat16)
    both_grads = both_cores(grad_here)
    both_normed_two = both_cores(normed_two)
    hidden_pre = jnp.dot(normed_two, full_up, preferred_element_type=jnp.float32)
    active = gelu_tanh(hidden_pre).astype(jnp.bfloat16)
    grad_out = grad_here.astype(jnp.float32)
    wdown_term = weight_term(both_grads, half_of_both(active, core))
    grad_here, wdown_term = lax.optimization_barrier((grad_here, wdown_term))
    wdown_rows = summed_rows(wdown_term)
    grad_active = jnp.dot(grad_here, full_down, preferred_element_type=jnp.float32)
    gelu_back = jax.vjp(gelu_tanh, hidden_pre)[1]
    grad_up = gelu_back(grad_active)[0].astype(jnp.bfloat16)
    norm_two_part = right_product(grad_up, full_up)
    wup_term = weight_term(both_normed_two, half_of_both(grad_up, core))
    grad_norm_two, wup_term = tensor_sum(norm_two_part, wup_term)
    wup_rows = summed_rows(wup_term)
    norm_two_back = jax.vjp(layer_norm, resid_mid, second_gain, second_shift)[1]
    grad_mid_norm, grad_gain_two, grad_shift_two = norm_two_back(grad_norm_two)
    grad_mid = grad_out + grad_mid_norm
    grad_mid_low = grad_mid.astype(jnp.bfloat16)
    grad_context = jnp.dot(grad_mid_low, full_out, preferred_element_type=jnp.float32)
    grad_context = grad_context.astype(jnp.bfloat16)
    grad_ctx_heads = grad_context.reshape(row_count, heads_here, head_dim)
    masked_again = masked_scores(query_heads, key_rows, visible, score_scale)
    probs_again = jnp.exp(masked_again - log_total)
    probs_low = probs_again.astype(jnp.bfloat16)
    grad_probs = jnp.einsum(
        "qhd,kd->hqk", grad_ctx_heads, value_rows, preferred_element_type=jnp.float32
    )
    row_delta = jnp.sum(grad_probs * probs_again, axis=2, keepdims=True)
    grad_scores = (probs_again * (grad_probs - row_delta)).astype(jnp.bfloat16)
    grad_query = (
        jnp.einsum("hqk,kd->qhd", grad_scores, key_rows, preferred_element_type=jnp.float32)
        * score_scale
    )
    grad_query = grad_query.reshape(row_count, heads_here * head_dim).astype(jnp.bfloat16)
    grad_keys = (
        jnp.einsum("hqk,qhd->kd", grad_scores, query_heads, preferred_element_type=jnp.float32)
        * score_scale
    )
    grad_values = jnp.einsum(
        "hqk,qhd->kd", probs_low, grad_ctx_heads, preferred_element_type=jnp.float32
    )
    grad_keyval_part = jnp.concatenate([grad_keys, grad_values], axis=1)
    grad_keyval_low = tensor_sum(grad_keyval_part).astype(jnp.bfloat16)
    grad_qkv_part = jnp.concatenate([grad_query, grad_keyval_part.astype(jnp.bfloat16)], axis=1)
    grad_norm_one = tensor_rows(right_product(grad_qkv_part, full_qkv), place)
    norm_one_back = jax.vjp(
        layer_norm, own_rows(resid_in, place, 2), first_gain, first_shift
    )[1]
    grad_in_norm, grad_gain_one, grad_shift_one = norm_one_back(grad_norm_one)
    grad_resid = (own_rows(grad_mid, place, 2) + grad_in_norm).astype(jnp.bfloat16)
    mlp_output = tensor_rows(right_product(active, full_down), place)
    result = (own_rows(resid_mid, place, 2) + mlp_output).astype(jnp.bfloat16)
    norm_one_sums = jnp.stack([grad_gain_one, grad_shift_one])
    norm_one_sums = norm_one_sums + swap_tensor(norm_one_sums)
    norm_sums = jnp.concatenate([norm_one_sums, jnp.stack([grad_gain_two, grad_shift_two])])
    norm_sums = norm_sums + swap_cores(norm_sums)
    grad_qkv = jnp.concatenate([grad_query, grad_keyval_low], axis=1)
    last_rows = summed_rows(
        jnp.concatenate(
            [
                weight_term(both_cores(normed_one), half_of_both(grad_qkv, core)),
                weight_term(both_cores(grad_mid_low), half_of_both(context, core)),
                as_columns((norm_sums[0], norm_sums[1], norm_sums[2], norm_sums[3])),
            ],
            axis=1,
        ),
    )
    qkv_half = qkv_cols // 2
    out_end = qkv_half + query_cols // 2
    grad_wdown = own_columns(wdown_rows, core)
    grad_wup = own_columns(wup_rows, core)
    grad_wqkv = own_columns(last_rows[:, :qkv_half], core)
    grad_wo = own_columns(last_rows[:, qkv_half:out_end], core)
    norm_grads = own_rows(last_rows[:, out_end : out_end + 4], core, 2).astype(jnp.float32).T
    restore = jnp.argsort(send_order.reshape(-1), stable=True)
    restore = lax.rem(restore + place * (row_count // 2), row_count)

    def returned(rows):
        mine = lax.all_to_all(rows, "dp", split_axis=0, concat_axis=0, tiled=True)
        return jnp.concatenate([mine, swap_tensor(mine)], axis=0)[restore]

    output = returned(result)
    grad_tokens = returned(grad_resid)
    return (
        output,
        grad_tokens,
        grad_wqkv[:, :query_cols],
        grad_wqkv[:, query_cols:],
        grad_wo,
        grad_wup,
        grad_wdown,
        norm_grads[0],
        norm_grads[1],
        norm_grads[2],
        norm_grads[3],
    )


def solution(mesh):
    placed = (
        P("dp", None),
        P("dp", None),
        P("dp", "tensor"),
        P("dp", None),
        P("dp", "tensor"),
        P("dp", "tensor"),
        P("dp", "tensor"),
        P("dp"),
        P("dp"),
        P("dp"),
        P("dp"),
        P(),
        P("dp", None),
    )

    return jax.shard_map(
        per_device,
        mesh=mesh,
        in_specs=placed,
        out_specs=(
            P("dp", None),
            P("dp", None),
            P("dp", "tensor"),
            P("dp", None),
            P("dp", "tensor"),
            P("dp", "tensor"),
            P("dp", "tensor"),
            P("dp"),
            P("dp"),
            P("dp"),
            P("dp"),
        ),
        check_vma=False,
    )
```

```python
import jax
import jax.numpy as jnp
from jax import lax
from jax.sharding import PartitionSpec as P

norm_eps = 1e-05


def layer_norm(values, gain_vector, shift_vector):
    row_mean = jnp.mean(values, axis=-1, keepdims=True)
    centered = values - row_mean
    spread = jnp.mean(centered * centered, axis=-1, keepdims=True)
    return centered * lax.rsqrt(spread + norm_eps) * gain_vector + shift_vector


def gelu_tanh(values):
    return jax.nn.gelu(values, approximate=True)


def visible_pairs(lengths_row, places):
    boundaries = jnp.cumsum(lengths_row)
    segment = jnp.sum((places[:, None] >= boundaries[None, :]).astype(jnp.int32), axis=1)
    return jnp.logical_and(segment[:, None] == segment[None, :], places[None, :] <= places[:, None])


def right_product(first_op, second_op):
    return lax.dot_general(
        first_op, second_op, (((1,), (1,)), ((), ())), preferred_element_type=jnp.float32
    )


def left_product(first_op, second_op):
    return lax.dot_general(
        first_op, second_op, (((0,), (0,)), ((), ())), preferred_element_type=jnp.float32
    )


def as_columns(vectors):
    columns = jnp.stack([vector.astype(jnp.bfloat16) for vector in vectors], axis=1)
    return jnp.pad(columns, ((0, 0), (0, 128 - len(vectors))))


def tensor_sum(values, ride_along=None):
    own = lax.optimization_barrier(values.astype(jnp.bfloat16))
    total = own.astype(jnp.float32)
    other = swap_tensor(own)
    if ride_along is not None:
        other, ride_along = lax.optimization_barrier((other, ride_along))
    summed = total + other.astype(jnp.float32)
    return summed if ride_along is None else (summed, ride_along)


def swap_cores(values):
    members = lax.axis_size("dp")
    return lax.ppermute(values, "dp", [(i, i ^ 1) for i in range(members)])


def column_half(values, half):
    width = values.shape[1] // 2
    return lax.dynamic_slice_in_dim(values, half * width, width, axis=1)


def own_rows(values, part, parts):
    count = values.shape[0] // parts
    return lax.dynamic_slice_in_dim(values, part * count, count, axis=0)


def both_cores(values):
    return jnp.concatenate([values, swap_cores(values)], axis=0)


def half_of_both(values, core):
    other = swap_cores(column_half(values, 1 - core))
    return jnp.concatenate([column_half(values, core), other], axis=0)


def summed_rows(low):
    members = lax.axis_size("dp")
    side = lax.rem(lax.axis_index("dp") // 2, 2)
    rows, cols = low.shape
    blocks = low.reshape(members // 4, 2, rows * 2 // members, cols)
    kept = lax.dynamic_index_in_dim(blocks, side, axis=1, keepdims=False)
    leaving = lax.dynamic_index_in_dim(blocks, 1 - side, axis=1, keepdims=False)
    other = lax.ppermute(leaving, "dp", [(i, i ^ 2) for i in range(members)])
    near = (kept.astype(jnp.float32) + other.astype(jnp.float32)).astype(jnp.bfloat16)
    groups = [list(range(first, members, 4)) for first in range(4)]
    return lax.psum_scatter(
        near.reshape(rows // 2, cols),
        "dp",
        scatter_dimension=0,
        axis_index_groups=groups,
        tiled=True,
    )


def own_columns(chip_rows, core):
    kept = own_rows(chip_rows, core, 2)
    other = swap_cores(own_rows(chip_rows, 1 - core, 2))
    first = jnp.where(core == 0, kept, other)
    second = jnp.where(core == 0, other, kept)
    return jnp.concatenate([first, second], axis=1).astype(jnp.float32)


def swap_tensor(values):
    return lax.ppermute(values, "tensor", [(0, 1), (1, 0)])


def tensor_rows(values, place):
    low = values.astype(jnp.bfloat16)
    arriving = swap_tensor(own_rows(low, 1 - place, 2))
    return own_rows(low, place, 2).astype(jnp.float32) + arriving.astype(jnp.float32)


def weight_term(first_op, second_op):
    return left_product(first_op, second_op).astype(jnp.bfloat16)


def masked_scores(query_heads, key_rows, visible, score_scale):
    scores = (
        jnp.einsum("qhd,kd->hqk", query_heads, key_rows, preferred_element_type=jnp.float32)
        * score_scale
    )
    return jnp.where(visible, scores, -1e30)


def per_device(
    tokens,
    cotangent,
    w_query,
    w_keyval,
    w_out,
    w_up,
    w_down,
    norm1_gain,
    norm1_bias,
    norm2_gain,
    norm2_bias,
    route,
    lengths,
):
    row_count = tokens.shape[0]
    head_dim = w_keyval.shape[1] // 2
    heads_here = w_query.shape[1] // head_dim
    score_scale = head_dim ** (-0.5)
    group_index = lax.axis_index("dp")
    groups = lax.axis_size("dp")
    core = lax.rem(group_index, 2)
    place = lax.axis_index("tensor")
    query_cols = w_query.shape[1]
    qkv_cols = query_cols + w_keyval.shape[1]
    up_cols = w_up.shape[1]
    full_attn = lax.all_gather(
        jnp.concatenate(
            [
                w_query.astype(jnp.bfloat16),
                w_keyval.astype(jnp.bfloat16),
                w_out.astype(jnp.bfloat16),
                as_columns((norm1_gain, norm1_bias, norm2_gain, norm2_bias)),
            ],
            axis=1,
        ),
        "dp",
        axis=0,
        tiled=True,
    )
    full_ffn = lax.all_gather(
        jnp.concatenate([w_up.astype(jnp.bfloat16), w_down.astype(jnp.bfloat16)], axis=1),
        "dp",
        axis=0,
        tiled=True,
    )
    full_up = full_ffn[:, :up_cols]
    full_down = full_ffn[:, up_cols:]

    def by_member(order):
        return order.reshape(groups, 2, -1).transpose(1, 0, 2)

    own_route = lax.dynamic_slice_in_dim(route, group_index * row_count, row_count)
    send_order = by_member(jnp.argsort(own_route, stable=True))
    own_sends = lax.dynamic_index_in_dim(send_order, place, keepdims=False).reshape(-1)

    def fetched(rows):
        mine = lax.all_to_all(rows[own_sends], "dp", split_axis=0, concat_axis=0, tiled=True)
        other = swap_tensor(mine)
        first = jnp.where(place == 0, mine, other)
        second = jnp.where(place == 0, other, mine)
        return jnp.concatenate([first, second], axis=0)

    tokens_here = fetched(tokens)
    grad_here = fetched(cotangent)
    inverse = jnp.argsort(route, stable=True)
    sources = lax.dynamic_slice_in_dim(inverse, group_index * row_count, row_count) // row_count
    places = by_member(jnp.argsort(sources, stable=True)).reshape(-1).astype(jnp.int32)
    full_qkv = full_attn[:, :qkv_cols]
    norm_at = qkv_cols + query_cols
    full_out = full_attn[:, qkv_cols:norm_at]
    norm_rows = full_attn[:, norm_at : norm_at + 4].astype(jnp.float32).T
    first_gain, first_shift, second_gain, second_shift = (
        norm_rows[0],
        norm_rows[1],
        norm_rows[2],
        norm_rows[3],
    )
    resid_in = tokens_here.astype(jnp.float32)
    normed_one = layer_norm(resid_in, first_gain, first_shift).astype(jnp.bfloat16)
    qkv = jnp.dot(normed_one, full_qkv, preferred_element_type=jnp.float32).astype(jnp.bfloat16)
    query_heads = qkv[:, :query_cols].reshape(row_count, heads_here, head_dim)
    key_rows = qkv[:, query_cols : query_cols + head_dim]
    value_rows = qkv[:, query_cols + head_dim :]
    visible = visible_pairs(lengths[0], places)[None]
    masked = masked_scores(query_heads, key_rows, visible, score_scale)
    row_max = jnp.max(masked, axis=2, keepdims=True)
    weights_exp = jnp.exp(masked - row_max)
    row_total = jnp.sum(weights_exp, axis=2, keepdims=True)
    probs_first = (weights_exp / row_total).astype(jnp.bfloat16)
    log_total = row_max + jnp.log(row_total)
    context = jnp.einsum("hqk,kd->qhd", probs_first, value_rows, preferred_element_type=jnp.float32)
    context = context.reshape(row_count, heads_here * head_dim).astype(jnp.bfloat16)
    attn_output = tensor_sum(right_product(context, full_out))
    resid_mid = resid_in + attn_output
    normed_two = layer_norm(resid_mid, second_gain, second_shift).astype(jnp.bfloat16)
    both_grads = both_cores(grad_here)
    both_normed_two = both_cores(normed_two)
    hidden_pre = jnp.dot(normed_two, full_up, preferred_element_type=jnp.float32)
    active = gelu_tanh(hidden_pre).astype(jnp.bfloat16)
    grad_out = grad_here.astype(jnp.float32)
    wdown_term = weight_term(both_grads, half_of_both(active, core))
    grad_here, wdown_term = lax.optimization_barrier((grad_here, wdown_term))
    wdown_rows = summed_rows(wdown_term)
    grad_active = jnp.dot(grad_here, full_down, preferred_element_type=jnp.float32)
    gelu_back = jax.vjp(gelu_tanh, hidden_pre)[1]
    grad_up = gelu_back(grad_active)[0].astype(jnp.bfloat16)
    norm_two_part = right_product(grad_up, full_up)
    wup_term = weight_term(both_normed_two, half_of_both(grad_up, core))
    mlp_part = right_product(active, full_down)
    grad_norm_two, wup_term = tensor_sum(norm_two_part, wup_term)
    wup_rows = summed_rows(wup_term)
    norm_two_back = jax.vjp(layer_norm, resid_mid, second_gain, second_shift)[1]
    grad_mid_norm, grad_gain_two, grad_shift_two = norm_two_back(grad_norm_two)
    grad_mid = grad_out + grad_mid_norm
    grad_mid_low = grad_mid.astype(jnp.bfloat16)
    grad_context = jnp.dot(grad_mid_low, full_out, preferred_element_type=jnp.float32)
    grad_context = grad_context.astype(jnp.bfloat16)
    grad_ctx_heads = grad_context.reshape(row_count, heads_here, head_dim)
    masked_again = masked_scores(query_heads, key_rows, visible, score_scale)
    probs_again = jnp.exp(masked_again - log_total)
    probs_low = probs_again.astype(jnp.bfloat16)
    grad_probs = jnp.einsum(
        "qhd,kd->hqk", grad_ctx_heads, value_rows, preferred_element_type=jnp.float32
    )
    row_delta = jnp.sum(grad_probs * probs_again, axis=2, keepdims=True)
    grad_scores = (probs_again * (grad_probs - row_delta)).astype(jnp.bfloat16)
    grad_query = (
        jnp.einsum("hqk,kd->qhd", grad_scores, key_rows, preferred_element_type=jnp.float32)
        * score_scale
    )
    grad_query = grad_query.reshape(row_count, heads_here * head_dim).astype(jnp.bfloat16)
    grad_keys = (
        jnp.einsum("hqk,qhd->kd", grad_scores, query_heads, preferred_element_type=jnp.float32)
        * score_scale
    )
    grad_values = jnp.einsum(
        "hqk,qhd->kd", probs_low, grad_ctx_heads, preferred_element_type=jnp.float32
    )
    grad_keyval_part = jnp.concatenate([grad_keys, grad_values], axis=1)
    grad_keyval_low = tensor_sum(grad_keyval_part).astype(jnp.bfloat16)
    grad_qkv_part = jnp.concatenate([grad_query, grad_keyval_part.astype(jnp.bfloat16)], axis=1)
    mlp_output = tensor_rows(mlp_part, place)
    result = (own_rows(resid_mid, place, 2) + mlp_output).astype(jnp.bfloat16)
    result, grad_qkv_part = lax.optimization_barrier((result, grad_qkv_part))
    output_rows = lax.all_to_all(result, "dp", split_axis=0, concat_axis=0, tiled=True)
    norm_one_part = right_product(grad_qkv_part, full_qkv)
    grad_norm_one = tensor_rows(norm_one_part, place)
    output_rows, grad_norm_one = lax.optimization_barrier((output_rows, grad_norm_one))
    norm_one_back = jax.vjp(
        layer_norm, own_rows(resid_in, place, 2), first_gain, first_shift
    )[1]
    grad_in_norm, grad_gain_one, grad_shift_one = norm_one_back(grad_norm_one)
    grad_resid = (own_rows(grad_mid, place, 2) + grad_in_norm).astype(jnp.bfloat16)
    norm_one_sums = jnp.stack([grad_gain_one, grad_shift_one])
    norm_one_sums = norm_one_sums + swap_tensor(norm_one_sums)
    norm_sums = jnp.concatenate([norm_one_sums, jnp.stack([grad_gain_two, grad_shift_two])])
    norm_sums = norm_sums + swap_cores(norm_sums)
    grad_qkv = jnp.concatenate([grad_query, grad_keyval_low], axis=1)
    last_rows = summed_rows(
        jnp.concatenate(
            [
                weight_term(both_cores(normed_one), half_of_both(grad_qkv, core)),
                weight_term(both_cores(grad_mid_low), half_of_both(context, core)),
                as_columns((norm_sums[0], norm_sums[1], norm_sums[2], norm_sums[3])),
            ],
            axis=1,
        ),
    )
    qkv_half = qkv_cols // 2
    out_end = qkv_half + query_cols // 2
    grad_wdown = own_columns(wdown_rows, core)
    grad_wup = own_columns(wup_rows, core)
    grad_wqkv = own_columns(last_rows[:, :qkv_half], core)
    grad_wo = own_columns(last_rows[:, qkv_half:out_end], core)
    norm_grads = own_rows(last_rows[:, out_end : out_end + 4], core, 2).astype(jnp.float32).T
    restore = jnp.argsort(send_order.reshape(-1), stable=True)
    restore = lax.rem(restore + place * (row_count // 2), row_count)

    def returned(mine):
        return jnp.concatenate([mine, swap_tensor(mine)], axis=0)[restore]

    output = returned(output_rows)
    grad_tokens = returned(
        lax.all_to_all(grad_resid, "dp", split_axis=0, concat_axis=0, tiled=True)
    )
    return (
        output,
        grad_tokens,
        grad_wqkv[:, :query_cols],
        grad_wqkv[:, query_cols:],
        grad_wo,
        grad_wup,
        grad_wdown,
        norm_grads[0],
        norm_grads[1],
        norm_grads[2],
        norm_grads[3],
    )


def solution(mesh):
    placed = (
        P("dp", None),
        P("dp", None),
        P("dp", "tensor"),
        P("dp", None),
        P("dp", "tensor"),
        P("dp", "tensor"),
        P("dp", "tensor"),
        P("dp"),
        P("dp"),
        P("dp"),
        P("dp"),
        P(),
        P("dp", None),
    )

    return jax.shard_map(
        per_device,
        mesh=mesh,
        in_specs=placed,
        out_specs=(
            P("dp", None),
            P("dp", None),
            P("dp", "tensor"),
            P("dp", None),
            P("dp", "tensor"),
            P("dp", "tensor"),
            P("dp", "tensor"),
            P("dp"),
            P("dp"),
            P("dp"),
            P("dp"),
        ),
        check_vma=False,
    )
```

```python
import jax
import jax.numpy as jnp
from jax import lax
from jax.sharding import PartitionSpec as P

norm_eps = 1e-05


def layer_norm(values, gain_vector, shift_vector):
    row_mean = jnp.mean(values, axis=-1, keepdims=True)
    centered = values - row_mean
    spread = jnp.mean(centered * centered, axis=-1, keepdims=True)
    return centered * lax.rsqrt(spread + norm_eps) * gain_vector + shift_vector


def gelu_tanh(values):
    return jax.nn.gelu(values, approximate=True)


def visible_pairs(lengths_row, places):
    boundaries = jnp.cumsum(lengths_row)
    segment = jnp.sum((places[:, None] >= boundaries[None, :]).astype(jnp.int32), axis=1)
    return jnp.logical_and(segment[:, None] == segment[None, :], places[None, :] <= places[:, None])


def right_product(first_op, second_op):
    return lax.dot_general(
        first_op, second_op, (((1,), (1,)), ((), ())), preferred_element_type=jnp.float32
    )


def left_product(first_op, second_op):
    return lax.dot_general(
        first_op, second_op, (((0,), (0,)), ((), ())), preferred_element_type=jnp.float32
    )


def as_columns(vectors):
    columns = jnp.stack([vector.astype(jnp.bfloat16) for vector in vectors], axis=1)
    return jnp.pad(columns, ((0, 0), (0, 128 - len(vectors))))


def tensor_sum(values, ride_along=None):
    own = lax.optimization_barrier(values.astype(jnp.bfloat16))
    total = own.astype(jnp.float32)
    other = swap_tensor(own)
    if ride_along is not None:
        other, ride_along = lax.optimization_barrier((other, ride_along))
    summed = total + other.astype(jnp.float32)
    return summed if ride_along is None else (summed, ride_along)


def swap_cores(values):
    members = lax.axis_size("dp")
    return lax.ppermute(values, "dp", [(i, i ^ 1) for i in range(members)])


def column_half(values, half):
    width = values.shape[1] // 2
    return lax.dynamic_slice_in_dim(values, half * width, width, axis=1)


def own_rows(values, part, parts):
    count = values.shape[0] // parts
    return lax.dynamic_slice_in_dim(values, part * count, count, axis=0)


def both_cores(values):
    return jnp.concatenate([values, swap_cores(values)], axis=0)


def half_of_both(values, core):
    other = swap_cores(column_half(values, 1 - core))
    return jnp.concatenate([column_half(values, core), other], axis=0)


def summed_rows(low):
    members = lax.axis_size("dp")
    groups = [list(range(core, members, 2)) for core in range(2)]
    return lax.psum_scatter(low, "dp", scatter_dimension=0, axis_index_groups=groups, tiled=True)


def own_columns(chip_rows, core):
    kept = own_rows(chip_rows, core, 2)
    other = swap_cores(own_rows(chip_rows, 1 - core, 2))
    first = jnp.where(core == 0, kept, other)
    second = jnp.where(core == 0, other, kept)
    return jnp.concatenate([first, second], axis=1).astype(jnp.float32)


def swap_tensor(values):
    return lax.ppermute(values, "tensor", [(0, 1), (1, 0)])


def tensor_rows(values, place):
    low = values.astype(jnp.bfloat16)
    arriving = swap_tensor(own_rows(low, 1 - place, 2))
    return own_rows(low, place, 2).astype(jnp.float32) + arriving.astype(jnp.float32)


def weight_term(first_op, second_op):
    return left_product(first_op, second_op).astype(jnp.bfloat16)


def masked_scores(query_heads, key_rows, visible, score_scale):
    scores = (
        jnp.einsum("qhd,kd->hqk", query_heads, key_rows, preferred_element_type=jnp.float32)
        * score_scale
    )
    return jnp.where(visible, scores, -1e30)


def per_device(
    tokens,
    cotangent,
    w_query,
    w_keyval,
    w_out,
    w_up,
    w_down,
    norm1_gain,
    norm1_bias,
    norm2_gain,
    norm2_bias,
    route,
    lengths,
):
    row_count = tokens.shape[0]
    head_dim = w_keyval.shape[1] // 2
    heads_here = w_query.shape[1] // head_dim
    score_scale = head_dim ** (-0.5)
    group_index = lax.axis_index("dp")
    groups = lax.axis_size("dp")
    core = lax.rem(group_index, 2)
    place = lax.axis_index("tensor")
    query_cols = w_query.shape[1]
    qkv_cols = query_cols + w_keyval.shape[1]
    up_cols = w_up.shape[1]
    full_attn = lax.all_gather(
        jnp.concatenate(
            [
                w_query.astype(jnp.bfloat16),
                w_keyval.astype(jnp.bfloat16),
                w_out.astype(jnp.bfloat16),
                as_columns((norm1_gain, norm1_bias, norm2_gain, norm2_bias)),
            ],
            axis=1,
        ),
        "dp",
        axis=0,
        tiled=True,
    )
    full_ffn = lax.all_gather(
        jnp.concatenate([w_up.astype(jnp.bfloat16), w_down.astype(jnp.bfloat16)], axis=1),
        "dp",
        axis=0,
        tiled=True,
    )
    full_up = full_ffn[:, :up_cols]
    full_down = full_ffn[:, up_cols:]

    def by_member(order):
        return order.reshape(groups, 2, -1).transpose(1, 0, 2)

    own_route = lax.dynamic_slice_in_dim(route, group_index * row_count, row_count)
    send_order = by_member(jnp.argsort(own_route, stable=True))
    own_sends = lax.dynamic_index_in_dim(send_order, place, keepdims=False).reshape(-1)

    def fetched(rows):
        mine = lax.all_to_all(rows[own_sends], "dp", split_axis=0, concat_axis=0, tiled=True)
        other = swap_tensor(mine)
        first = jnp.where(place == 0, mine, other)
        second = jnp.where(place == 0, other, mine)
        return jnp.concatenate([first, second], axis=0)

    tokens_here = fetched(tokens)
    grad_here = fetched(cotangent)
    inverse = jnp.argsort(route, stable=True)
    sources = lax.dynamic_slice_in_dim(inverse, group_index * row_count, row_count) // row_count
    places = by_member(jnp.argsort(sources, stable=True)).reshape(-1).astype(jnp.int32)
    full_qkv = full_attn[:, :qkv_cols]
    norm_at = qkv_cols + query_cols
    full_out = full_attn[:, qkv_cols:norm_at]
    norm_rows = full_attn[:, norm_at : norm_at + 4].astype(jnp.float32).T
    first_gain, first_shift, second_gain, second_shift = (
        norm_rows[0],
        norm_rows[1],
        norm_rows[2],
        norm_rows[3],
    )
    resid_in = tokens_here.astype(jnp.float32)
    normed_one = layer_norm(resid_in, first_gain, first_shift).astype(jnp.bfloat16)
    qkv = jnp.dot(normed_one, full_qkv, preferred_element_type=jnp.float32).astype(jnp.bfloat16)
    query_heads = qkv[:, :query_cols].reshape(row_count, heads_here, head_dim)
    key_rows = qkv[:, query_cols : query_cols + head_dim]
    value_rows = qkv[:, query_cols + head_dim :]
    visible = visible_pairs(lengths[0], places)[None]
    masked = masked_scores(query_heads, key_rows, visible, score_scale)
    row_max = jnp.max(masked, axis=2, keepdims=True)
    weights_exp = jnp.exp(masked - row_max)
    row_total = jnp.sum(weights_exp, axis=2, keepdims=True)
    probs_first = (weights_exp / row_total).astype(jnp.bfloat16)
    log_total = row_max + jnp.log(row_total)
    context = jnp.einsum("hqk,kd->qhd", probs_first, value_rows, preferred_element_type=jnp.float32)
    context = context.reshape(row_count, heads_here * head_dim).astype(jnp.bfloat16)
    attn_output = tensor_sum(right_product(context, full_out))
    resid_mid = resid_in + attn_output
    normed_two = layer_norm(resid_mid, second_gain, second_shift).astype(jnp.bfloat16)
    both_grads = both_cores(grad_here)
    both_normed_two = both_cores(normed_two)
    hidden_pre = jnp.dot(normed_two, full_up, preferred_element_type=jnp.float32)
    active = gelu_tanh(hidden_pre).astype(jnp.bfloat16)
    grad_out = grad_here.astype(jnp.float32)
    wdown_term = weight_term(both_grads, half_of_both(active, core))
    grad_here, wdown_term = lax.optimization_barrier((grad_here, wdown_term))
    wdown_rows = summed_rows(wdown_term)
    grad_active = jnp.dot(grad_here, full_down, preferred_element_type=jnp.float32)
    gelu_back = jax.vjp(gelu_tanh, hidden_pre)[1]
    grad_up = gelu_back(grad_active)[0].astype(jnp.bfloat16)
    norm_two_part = right_product(grad_up, full_up)
    wup_term = weight_term(both_normed_two, half_of_both(grad_up, core))
    mlp_part = right_product(active, full_down)
    grad_norm_two, wup_term = tensor_sum(norm_two_part, wup_term)
    wup_rows = summed_rows(wup_term)
    norm_two_back = jax.vjp(layer_norm, resid_mid, second_gain, second_shift)[1]
    grad_mid_norm, grad_gain_two, grad_shift_two = norm_two_back(grad_norm_two)
    grad_mid = grad_out + grad_mid_norm
    grad_mid_low = grad_mid.astype(jnp.bfloat16)
    grad_context = jnp.dot(grad_mid_low, full_out, preferred_element_type=jnp.float32)
    grad_context = grad_context.astype(jnp.bfloat16)
    grad_ctx_heads = grad_context.reshape(row_count, heads_here, head_dim)
    masked_again = masked_scores(query_heads, key_rows, visible, score_scale)
    probs_again = jnp.exp(masked_again - log_total)
    probs_low = probs_again.astype(jnp.bfloat16)
    grad_probs = jnp.einsum(
        "qhd,kd->hqk", grad_ctx_heads, value_rows, preferred_element_type=jnp.float32
    )
    row_delta = jnp.sum(grad_probs * probs_again, axis=2, keepdims=True)
    grad_scores = (probs_again * (grad_probs - row_delta)).astype(jnp.bfloat16)
    grad_query = (
        jnp.einsum("hqk,kd->qhd", grad_scores, key_rows, preferred_element_type=jnp.float32)
        * score_scale
    )
    grad_query = grad_query.reshape(row_count, heads_here * head_dim).astype(jnp.bfloat16)
    grad_keys = (
        jnp.einsum("hqk,qhd->kd", grad_scores, query_heads, preferred_element_type=jnp.float32)
        * score_scale
    )
    grad_values = jnp.einsum(
        "hqk,qhd->kd", probs_low, grad_ctx_heads, preferred_element_type=jnp.float32
    )
    grad_keyval_part = jnp.concatenate([grad_keys, grad_values], axis=1)
    grad_keyval_low = tensor_sum(grad_keyval_part).astype(jnp.bfloat16)
    grad_qkv_part = jnp.concatenate([grad_query, grad_keyval_part.astype(jnp.bfloat16)], axis=1)
    mlp_output = tensor_rows(mlp_part, place)
    result = (own_rows(resid_mid, place, 2) + mlp_output).astype(jnp.bfloat16)
    result, grad_qkv_part = lax.optimization_barrier((result, grad_qkv_part))
    output_rows = lax.all_to_all(result, "dp", split_axis=0, concat_axis=0, tiled=True)
    norm_one_part = right_product(grad_qkv_part, full_qkv)
    grad_norm_one = tensor_rows(norm_one_part, place)
    output_rows, grad_norm_one = lax.optimization_barrier((output_rows, grad_norm_one))
    norm_one_back = jax.vjp(
        layer_norm, own_rows(resid_in, place, 2), first_gain, first_shift
    )[1]
    grad_in_norm, grad_gain_one, grad_shift_one = norm_one_back(grad_norm_one)
    grad_resid = (own_rows(grad_mid, place, 2) + grad_in_norm).astype(jnp.bfloat16)
    norm_one_sums = jnp.stack([grad_gain_one, grad_shift_one])
    norm_one_sums = norm_one_sums + swap_tensor(norm_one_sums)
    norm_sums = jnp.concatenate([norm_one_sums, jnp.stack([grad_gain_two, grad_shift_two])])
    norm_sums = norm_sums + swap_cores(norm_sums)
    grad_qkv = jnp.concatenate([grad_query, grad_keyval_low], axis=1)
    last_rows = summed_rows(
        jnp.concatenate(
            [
                weight_term(both_cores(normed_one), half_of_both(grad_qkv, core)),
                weight_term(both_cores(grad_mid_low), half_of_both(context, core)),
                as_columns((norm_sums[0], norm_sums[1], norm_sums[2], norm_sums[3])),
            ],
            axis=1,
        ),
    )
    qkv_half = qkv_cols // 2
    out_end = qkv_half + query_cols // 2
    grad_wdown = own_columns(wdown_rows, core)
    grad_wup = own_columns(wup_rows, core)
    grad_wqkv = own_columns(last_rows[:, :qkv_half], core)
    grad_wo = own_columns(last_rows[:, qkv_half:out_end], core)
    norm_grads = own_rows(last_rows[:, out_end : out_end + 4], core, 2).astype(jnp.float32).T
    restore = jnp.argsort(send_order.reshape(-1), stable=True)
    restore = lax.rem(restore + place * (row_count // 2), row_count)

    def returned(mine):
        return jnp.concatenate([mine, swap_tensor(mine)], axis=0)[restore]

    output = returned(output_rows)
    grad_tokens = returned(
        lax.all_to_all(grad_resid, "dp", split_axis=0, concat_axis=0, tiled=True)
    )
    return (
        output,
        grad_tokens,
        grad_wqkv[:, :query_cols],
        grad_wqkv[:, query_cols:],
        grad_wo,
        grad_wup,
        grad_wdown,
        norm_grads[0],
        norm_grads[1],
        norm_grads[2],
        norm_grads[3],
    )


def solution(mesh):
    placed = (
        P("dp", None),
        P("dp", None),
        P("dp", "tensor"),
        P("dp", None),
        P("dp", "tensor"),
        P("dp", "tensor"),
        P("dp", "tensor"),
        P("dp"),
        P("dp"),
        P("dp"),
        P("dp"),
        P(),
        P("dp", None),
    )

    return jax.shard_map(
        per_device,
        mesh=mesh,
        in_specs=placed,
        out_specs=(
            P("dp", None),
            P("dp", None),
            P("dp", "tensor"),
            P("dp", None),
            P("dp", "tensor"),
            P("dp", "tensor"),
            P("dp", "tensor"),
            P("dp"),
            P("dp"),
            P("dp"),
            P("dp"),
        ),
        check_vma=False,
    )
```

```python
import jax
import jax.numpy as jnp
from jax import lax
from jax.sharding import PartitionSpec as P

norm_eps = 1e-05


def layer_norm(values, gain_vector, shift_vector):
    row_mean = jnp.mean(values, axis=-1, keepdims=True)
    centered = values - row_mean
    spread = jnp.mean(centered * centered, axis=-1, keepdims=True)
    return centered * lax.rsqrt(spread + norm_eps) * gain_vector + shift_vector


def gelu_tanh(values):
    return jax.nn.gelu(values, approximate=True)


def visible_pairs(lengths_row, places):
    boundaries = jnp.cumsum(lengths_row)
    segment = jnp.sum((places[:, None] >= boundaries[None, :]).astype(jnp.int32), axis=1)
    return jnp.logical_and(segment[:, None] == segment[None, :], places[None, :] <= places[:, None])


def right_product(first_op, second_op):
    return lax.dot_general(
        first_op, second_op, (((1,), (1,)), ((), ())), preferred_element_type=jnp.float32
    )


def left_product(first_op, second_op):
    return lax.dot_general(
        first_op, second_op, (((0,), (0,)), ((), ())), preferred_element_type=jnp.float32
    )


def as_columns(vectors):
    columns = jnp.stack([vector.astype(jnp.bfloat16) for vector in vectors], axis=1)
    return jnp.pad(columns, ((0, 0), (0, 128 - len(vectors))))


def tensor_sum(values, ride_along=None):
    own = lax.optimization_barrier(values.astype(jnp.bfloat16))
    total = own.astype(jnp.float32)
    other = swap_tensor(own)
    if ride_along is not None:
        other, ride_along = lax.optimization_barrier((other, ride_along))
    summed = total + other.astype(jnp.float32)
    return summed if ride_along is None else (summed, ride_along)


def swap_cores(values):
    members = lax.axis_size("dp")
    return lax.ppermute(values, "dp", [(i, i ^ 1) for i in range(members)])


def column_half(values, half):
    width = values.shape[1] // 2
    return lax.dynamic_slice_in_dim(values, half * width, width, axis=1)


def own_rows(values, part, parts):
    count = values.shape[0] // parts
    return lax.dynamic_slice_in_dim(values, part * count, count, axis=0)


def both_cores(values):
    return jnp.concatenate([values, swap_cores(values)], axis=0)


def half_of_both(values, core):
    other = swap_cores(column_half(values, 1 - core))
    return jnp.concatenate([column_half(values, core), other], axis=0)


def summed_rows(low):
    members = lax.axis_size("dp")
    groups = [list(range(core, members, 2)) for core in range(2)]
    return lax.psum_scatter(low, "dp", scatter_dimension=0, axis_index_groups=groups, tiled=True)


def near_sum(low):
    members = lax.axis_size("dp")
    side = lax.rem(lax.axis_index("dp") // 2, 2)
    rows, cols = low.shape
    blocks = low.reshape(members // 4, 2, rows * 2 // members, cols)
    leaving = lax.dynamic_index_in_dim(blocks, 1 - side, axis=1, keepdims=False)
    other = lax.ppermute(leaving, "dp", [(i, i ^ 2) for i in range(members)])
    kept = lax.dynamic_index_in_dim(blocks, side, axis=1, keepdims=False)
    near = kept.astype(jnp.float32) + other.astype(jnp.float32)
    return near.astype(jnp.bfloat16).reshape(rows // 2, cols)


def far_rows(near):
    members = lax.axis_size("dp")
    groups = [list(range(first, members, 4)) for first in range(4)]
    return lax.psum_scatter(near, "dp", scatter_dimension=0, axis_index_groups=groups, tiled=True)


def own_columns(chip_rows, core):
    kept = own_rows(chip_rows, core, 2)
    other = swap_cores(own_rows(chip_rows, 1 - core, 2))
    first = jnp.where(core == 0, kept, other)
    second = jnp.where(core == 0, other, kept)
    return jnp.concatenate([first, second], axis=1).astype(jnp.float32)


def swap_tensor(values):
    return lax.ppermute(values, "tensor", [(0, 1), (1, 0)])


def tensor_rows(values, place):
    low = values.astype(jnp.bfloat16)
    arriving = swap_tensor(own_rows(low, 1 - place, 2))
    return own_rows(low, place, 2).astype(jnp.float32) + arriving.astype(jnp.float32)


def weight_term(first_op, second_op):
    return left_product(first_op, second_op).astype(jnp.bfloat16)


def masked_scores(query_heads, key_rows, visible, score_scale):
    scores = (
        jnp.einsum("qhd,kd->hqk", query_heads, key_rows, preferred_element_type=jnp.float32)
        * score_scale
    )
    return jnp.where(visible, scores, -1e30)


def per_device(
    tokens,
    cotangent,
    w_query,
    w_keyval,
    w_out,
    w_up,
    w_down,
    norm1_gain,
    norm1_bias,
    norm2_gain,
    norm2_bias,
    route,
    lengths,
):
    row_count = tokens.shape[0]
    head_dim = w_keyval.shape[1] // 2
    heads_here = w_query.shape[1] // head_dim
    score_scale = head_dim ** (-0.5)
    group_index = lax.axis_index("dp")
    groups = lax.axis_size("dp")
    core = lax.rem(group_index, 2)
    place = lax.axis_index("tensor")
    query_cols = w_query.shape[1]
    qkv_cols = query_cols + w_keyval.shape[1]
    up_cols = w_up.shape[1]
    full_attn = lax.all_gather(
        jnp.concatenate(
            [
                w_query.astype(jnp.bfloat16),
                w_keyval.astype(jnp.bfloat16),
                w_out.astype(jnp.bfloat16),
                as_columns((norm1_gain, norm1_bias, norm2_gain, norm2_bias)),
            ],
            axis=1,
        ),
        "dp",
        axis=0,
        tiled=True,
    )
    full_ffn = lax.all_gather(
        jnp.concatenate([w_up.astype(jnp.bfloat16), w_down.astype(jnp.bfloat16)], axis=1),
        "dp",
        axis=0,
        tiled=True,
    )
    full_up = full_ffn[:, :up_cols]
    full_down = full_ffn[:, up_cols:]

    def by_member(order):
        return order.reshape(groups, 2, -1).transpose(1, 0, 2)

    own_route = lax.dynamic_slice_in_dim(route, group_index * row_count, row_count)
    send_order = by_member(jnp.argsort(own_route, stable=True))
    own_sends = lax.dynamic_index_in_dim(send_order, place, keepdims=False).reshape(-1)

    def fetched(rows):
        mine = lax.all_to_all(rows[own_sends], "dp", split_axis=0, concat_axis=0, tiled=True)
        other = swap_tensor(mine)
        first = jnp.where(place == 0, mine, other)
        second = jnp.where(place == 0, other, mine)
        return jnp.concatenate([first, second], axis=0)

    tokens_here = fetched(tokens)
    grad_here = fetched(cotangent)
    inverse = jnp.argsort(route, stable=True)
    sources = lax.dynamic_slice_in_dim(inverse, group_index * row_count, row_count) // row_count
    places = by_member(jnp.argsort(sources, stable=True)).reshape(-1).astype(jnp.int32)
    full_qkv = full_attn[:, :qkv_cols]
    norm_at = qkv_cols + query_cols
    full_out = full_attn[:, qkv_cols:norm_at]
    norm_rows = full_attn[:, norm_at : norm_at + 4].astype(jnp.float32).T
    first_gain, first_shift, second_gain, second_shift = (
        norm_rows[0],
        norm_rows[1],
        norm_rows[2],
        norm_rows[3],
    )
    resid_in = tokens_here.astype(jnp.float32)
    normed_one = layer_norm(resid_in, first_gain, first_shift).astype(jnp.bfloat16)
    qkv = jnp.dot(normed_one, full_qkv, preferred_element_type=jnp.float32).astype(jnp.bfloat16)
    query_heads = qkv[:, :query_cols].reshape(row_count, heads_here, head_dim)
    key_rows = qkv[:, query_cols : query_cols + head_dim]
    value_rows = qkv[:, query_cols + head_dim :]
    visible = visible_pairs(lengths[0], places)[None]
    masked = masked_scores(query_heads, key_rows, visible, score_scale)
    row_max = jnp.max(masked, axis=2, keepdims=True)
    weights_exp = jnp.exp(masked - row_max)
    row_total = jnp.sum(weights_exp, axis=2, keepdims=True)
    probs_first = (weights_exp / row_total).astype(jnp.bfloat16)
    log_total = row_max + jnp.log(row_total)
    context = jnp.einsum("hqk,kd->qhd", probs_first, value_rows, preferred_element_type=jnp.float32)
    context = context.reshape(row_count, heads_here * head_dim).astype(jnp.bfloat16)
    attn_output = tensor_sum(right_product(context, full_out))
    resid_mid = resid_in + attn_output
    normed_two = layer_norm(resid_mid, second_gain, second_shift).astype(jnp.bfloat16)
    both_grads = both_cores(grad_here)
    both_normed_two = both_cores(normed_two)
    hidden_pre = jnp.dot(normed_two, full_up, preferred_element_type=jnp.float32)
    active = gelu_tanh(hidden_pre).astype(jnp.bfloat16)
    grad_out = grad_here.astype(jnp.float32)
    wdown_term = weight_term(both_grads, half_of_both(active, core))
    grad_here, wdown_term = lax.optimization_barrier((grad_here, wdown_term))
    wdown_rows = summed_rows(wdown_term)
    grad_active = jnp.dot(grad_here, full_down, preferred_element_type=jnp.float32)
    gelu_back = jax.vjp(gelu_tanh, hidden_pre)[1]
    grad_up = gelu_back(grad_active)[0].astype(jnp.bfloat16)
    norm_two_part = right_product(grad_up, full_up)
    both_grad_up = half_of_both(grad_up, core)
    wup_term = weight_term(both_normed_two, both_grad_up)
    mlp_part = right_product(active, full_down)
    grad_norm_two = tensor_sum(norm_two_part)
    wup_rows = far_rows(near_sum(wup_term))
    norm_two_back = jax.vjp(layer_norm, resid_mid, second_gain, second_shift)[1]
    grad_mid_norm, grad_gain_two, grad_shift_two = norm_two_back(grad_norm_two)
    grad_mid = grad_out + grad_mid_norm
    grad_mid_low = grad_mid.astype(jnp.bfloat16)
    grad_context = jnp.dot(grad_mid_low, full_out, preferred_element_type=jnp.float32)
    grad_context = grad_context.astype(jnp.bfloat16)
    grad_ctx_heads = grad_context.reshape(row_count, heads_here, head_dim)
    masked_again = masked_scores(query_heads, key_rows, visible, score_scale)
    probs_again = jnp.exp(masked_again - log_total)
    probs_low = probs_again.astype(jnp.bfloat16)
    grad_probs = jnp.einsum(
        "qhd,kd->hqk", grad_ctx_heads, value_rows, preferred_element_type=jnp.float32
    )
    row_delta = jnp.sum(grad_probs * probs_again, axis=2, keepdims=True)
    grad_scores = (probs_again * (grad_probs - row_delta)).astype(jnp.bfloat16)
    grad_query = (
        jnp.einsum("hqk,kd->qhd", grad_scores, key_rows, preferred_element_type=jnp.float32)
        * score_scale
    )
    grad_query = grad_query.reshape(row_count, heads_here * head_dim).astype(jnp.bfloat16)
    grad_keys = (
        jnp.einsum("hqk,qhd->kd", grad_scores, query_heads, preferred_element_type=jnp.float32)
        * score_scale
    )
    grad_values = jnp.einsum(
        "hqk,qhd->kd", probs_low, grad_ctx_heads, preferred_element_type=jnp.float32
    )
    grad_keyval_part = jnp.concatenate([grad_keys, grad_values], axis=1)
    grad_keyval_low = tensor_sum(grad_keyval_part).astype(jnp.bfloat16)
    grad_qkv_part = jnp.concatenate([grad_query, grad_keyval_part.astype(jnp.bfloat16)], axis=1)
    mlp_output = tensor_rows(mlp_part, place)
    result = (own_rows(resid_mid, place, 2) + mlp_output).astype(jnp.bfloat16)
    result, grad_qkv_part = lax.optimization_barrier((result, grad_qkv_part))
    output_rows = lax.all_to_all(result, "dp", split_axis=0, concat_axis=0, tiled=True)
    norm_one_part = right_product(grad_qkv_part, full_qkv)
    grad_norm_one = tensor_rows(norm_one_part, place)
    output_rows, grad_norm_one = lax.optimization_barrier((output_rows, grad_norm_one))
    norm_one_back = jax.vjp(
        layer_norm, own_rows(resid_in, place, 2), first_gain, first_shift
    )[1]
    grad_in_norm, grad_gain_one, grad_shift_one = norm_one_back(grad_norm_one)
    grad_resid = (own_rows(grad_mid, place, 2) + grad_in_norm).astype(jnp.bfloat16)
    norm_one_sums = jnp.stack([grad_gain_one, grad_shift_one])
    norm_one_sums = norm_one_sums + swap_tensor(norm_one_sums)
    norm_sums = jnp.concatenate([norm_one_sums, jnp.stack([grad_gain_two, grad_shift_two])])
    norm_sums = norm_sums + swap_cores(norm_sums)
    grad_qkv = jnp.concatenate([grad_query, grad_keyval_low], axis=1)
    last_rows = summed_rows(
        jnp.concatenate(
            [
                weight_term(both_cores(normed_one), half_of_both(grad_qkv, core)),
                weight_term(both_cores(grad_mid_low), half_of_both(context, core)),
                as_columns((norm_sums[0], norm_sums[1], norm_sums[2], norm_sums[3])),
            ],
            axis=1,
        ),
    )
    qkv_half = qkv_cols // 2
    out_end = qkv_half + query_cols // 2
    grad_wdown = own_columns(wdown_rows, core)
    grad_wup = own_columns(wup_rows, core)
    grad_wqkv = own_columns(last_rows[:, :qkv_half], core)
    grad_wo = own_columns(last_rows[:, qkv_half:out_end], core)
    norm_grads = own_rows(last_rows[:, out_end : out_end + 4], core, 2).astype(jnp.float32).T
    restore = jnp.argsort(send_order.reshape(-1), stable=True)
    restore = lax.rem(restore + place * (row_count // 2), row_count)

    def returned(mine):
        return jnp.concatenate([mine, swap_tensor(mine)], axis=0)[restore]

    output = returned(output_rows)
    grad_tokens = returned(
        lax.all_to_all(grad_resid, "dp", split_axis=0, concat_axis=0, tiled=True)
    )
    return (
        output,
        grad_tokens,
        grad_wqkv[:, :query_cols],
        grad_wqkv[:, query_cols:],
        grad_wo,
        grad_wup,
        grad_wdown,
        norm_grads[0],
        norm_grads[1],
        norm_grads[2],
        norm_grads[3],
    )


def solution(mesh):
    placed = (
        P("dp", None),
        P("dp", None),
        P("dp", "tensor"),
        P("dp", None),
        P("dp", "tensor"),
        P("dp", "tensor"),
        P("dp", "tensor"),
        P("dp"),
        P("dp"),
        P("dp"),
        P("dp"),
        P(),
        P("dp", None),
    )

    return jax.shard_map(
        per_device,
        mesh=mesh,
        in_specs=placed,
        out_specs=(
            P("dp", None),
            P("dp", None),
            P("dp", "tensor"),
            P("dp", None),
            P("dp", "tensor"),
            P("dp", "tensor"),
            P("dp", "tensor"),
            P("dp"),
            P("dp"),
            P("dp"),
            P("dp"),
        ),
        check_vma=False,
    )
```
